32 devices in a mesh: prow: 4 (over y, x), pcol: 8 (over z, core).
Axes of the slice: x: 2, y: 2, z: 4, core: 2. Of those that a mesh axis runs over, the one named last changes fastest.
Arguments:
- matrix: float32 [16, 4, 256, 8, 8, 256], P(None, 'prow', None, None, 'pcol'), may hold values from -6 to 6, as said below
- factor: float32 [16, 4, 256, 8, 8, 256], P(None, 'prow', None, None, 'pcol'), may hold values from -3 to 3, as said below
Outputs:
- reduced: float32 [16, 4, 256, 8, 8, 256], P(None, 'prow', None, None, 'pcol')
The draws below stay inside these ranges and needn't reach their ends.
Inputs may be any that keep to these rules, and one draw needn't show every extreme that they name: Symmetric matrix stored in its lower triangle: every entry above the diagonal is zero. `factor`: lower triangular with diagonal entries between 1 and 3; every entry above the diagonal is zero.
All inputs are finite; a program needn't handle non-finite values.
Results may differ from the reference program's by a relative error of at most 0.0001.
Values sent between devices are 32-bit elements; how exact they have to be, the bound alone decides.
A program may use at most 256 MiB of HBM per device.

```python
import jax
import jax.numpy as jnp
from jax import lax

ORDER = 16384
NB = 256
BLOCKS = 2
RT = 16
CT = 8


def draw_matrix(key, part):
    rows = jnp.arange(ORDER, dtype=jnp.int32)[:, None]
    cols = jnp.arange(ORDER, dtype=jnp.int32)[None, :]
    values = jnp.clip(jax.random.normal(key, (ORDER, ORDER), jnp.float32), -6.0, 6.0)
    values = jnp.where(rows >= cols, values, 0.0)
    return values.reshape(RT, ORDER // (RT * NB), NB, CT, ORDER // (CT * NB), NB)


def draw_factor(key, part):
    first, second = jax.random.split(jax.random.fold_in(key, 7))
    rows = jnp.arange(ORDER, dtype=jnp.int32)[:, None]
    cols = jnp.arange(ORDER, dtype=jnp.int32)[None, :]
    same_tile = rows // NB == cols // NB
    spread = jnp.where(same_tile, 0.5, 0.3) / jnp.sqrt(jnp.float32(NB))
    noise = jnp.clip(jax.random.normal(first, (ORDER, ORDER), jnp.float32), -5.0, 5.0)
    diagonal = jnp.exp(jax.random.uniform(second, (ORDER,), jnp.float32, 0.0, jnp.log(3.0)))
    values = jnp.where(rows > cols, noise * spread, 0.0) + jnp.where(rows == cols, diagonal[:, None], 0.0)
    return values.reshape(RT, ORDER // (RT * NB), NB, CT, ORDER // (CT * NB), NB)


def setup_inputs(seed: int = 0) -> dict:
    keys = jax.random.split(jax.random.key(seed), 3)
    return {
        "matrix": draw_matrix(jax.random.fold_in(keys[2], 71), 0),
        "factor": draw_factor(jax.random.fold_in(keys[2], 71), 0),
    }


highest = lax.Precision.HIGHEST

def product(left, right):
    return jnp.dot(left.astype(jnp.float32), right.astype(jnp.float32), precision=highest, preferred_element_type=jnp.float32)

def product_trans(left, right):
    return lax.dot_general(left.astype(jnp.float32), right.astype(jnp.float32), (((1,), (1,)), ((), ())), precision=highest, preferred_element_type=jnp.float32)

def diagonal_core(diag_block, diag_factor, width):
    identity = jnp.eye(width, dtype=jnp.float32)
    inverse = lax.linalg.triangular_solve(diag_factor, identity, left_side=True, lower=True)
    symmetric = diag_block + diag_block.T - jnp.diag(jnp.diagonal(diag_block))
    inner = product_trans(product(inverse, symmetric), inverse)
    return (inverse, 0.5 * (inner + inner.T))

def reference(matrix, factor):
    full = matrix.reshape(ORDER, ORDER)
    lower = factor.reshape(ORDER, ORDER)
    for step in range(BLOCKS):
        low = step * NB
        high = low + NB
        inverse, core = diagonal_core(full[low:high, low:high], lower[low:high, low:high], NB)
        panel = full[high:, low:high]
        factor_panel = lower[high:, low:high]
        shared = product(factor_panel, core)
        halfway = product_trans(panel, inverse) - 0.5 * shared
        finished = halfway - 0.5 * shared
        update = product_trans(halfway, factor_panel) + product_trans(factor_panel, halfway)
        trailing = full[high:, high:] - jnp.tril(update)
        full = full.at[high:, high:].set(trailing)
        full = full.at[low:high, low:high].set(jnp.tril(core))
        full = full.at[high:, low:high].set(finished)
    return full.reshape(RT, ORDER // (RT * NB), NB, CT, ORDER // (CT * NB), NB)
```

```python
import jax
import jax.numpy as jnp
from jax import lax
from jax.sharding import PartitionSpec as P

BLOCKS = 2
BASE = 16

highest = lax.Precision.HIGHEST
high = lax.Precision.HIGH


def product(left, right):
    return jnp.dot(left, right, precision=highest, preferred_element_type=jnp.float32)


def product_trans(left, right, precision=highest):
    return lax.dot_general(
        left, right, (((1,), (1,)), ((), ())), precision=precision, preferred_element_type=jnp.float32
    )


def batched(left, right):
    return jnp.einsum("bij,bjk->bik", left, right, precision=highest, preferred_element_type=jnp.float32)


def invert(lower):
    count, width, _ = lower.shape
    size = BASE if width % BASE == 0 else width

    def blocks(extent, row, col):
        return lower[:, row * extent : (row + 1) * extent, col * extent : (col + 1) * extent]

    parts = width // size
    diag = jnp.stack([blocks(size, i, i) for i in range(parts)], 1).reshape(count * parts, size, size)
    rows = jnp.arange(size)[None, :, None]
    result = jnp.broadcast_to(jnp.eye(size, dtype=jnp.float32), diag.shape)
    for i in range(size):
        pivot = result[:, i : i + 1, :] / diag[:, i : i + 1, i : i + 1]
        changed = jnp.where(rows > i, result - diag[:, :, i : i + 1] * pivot, result)
        result = lax.optimization_barrier(jnp.where(rows == i, pivot, changed))
    while parts > 1:
        pairs = parts // 2
        split = result.reshape(count * pairs, 2, size, size)
        upper, under = split[:, 0], split[:, 1]
        cross = jnp.stack([blocks(size, 2 * j + 1, 2 * j) for j in range(pairs)], 1)
        cross = cross.reshape(count * pairs, size, size)
        corner = -batched(batched(under, cross), upper)
        top = jnp.concatenate([upper, jnp.zeros_like(upper)], 2)
        result = jnp.concatenate([top, jnp.concatenate([corner, under], 2)], 1)
        parts, size = pairs, 2 * size
    return result.reshape(count, width, width)


def core_of(block, inverse):
    symmetric = block + block.T - jnp.diag(jnp.diagonal(block))
    inner = product_trans(product(inverse, symmetric), inverse)
    return 0.5 * (inner + inner.T)


def on_device(matrix, factor):
    row_tiles = matrix.shape[0]
    width = matrix.shape[2]
    col_tiles = matrix.shape[3]
    prow_count = lax.axis_size("prow")
    pcol_count = lax.axis_size("pcol")
    prow_index = lax.axis_index("prow")
    pcol_index = lax.axis_index("pcol")
    height = row_tiles * width
    breadth = col_tiles * width
    tile_rows = jnp.arange(row_tiles, dtype=jnp.int32) * prow_count + prow_index
    tile_cols = jnp.arange(col_tiles, dtype=jnp.int32) * pcol_count + pcol_index
    offsets = jnp.arange(width, dtype=jnp.int32)
    elem_rows = (tile_rows[:, None] * width + offsets[None, :]).reshape(height)
    elem_cols = (tile_cols[:, None] * width + offsets[None, :]).reshape(breadth)
    row_tile_of = jnp.repeat(tile_rows, width)[:, None]
    col_tile_of = jnp.repeat(tile_cols, width)[:, None]
    ratio = pcol_count // prow_count
    keeper = prow_index == pcol_index % prow_count

    raw = []
    for step in range(BLOCKS):
        place = step // pcol_count
        raw.append((matrix[:, 0, :, place, 0, :], factor[:, 0, :, place, 0, :]))

    wanted = []
    for tile in range(BLOCKS):
        for step in range(tile + 1):
            held = (prow_index == tile % prow_count) & (pcol_index == step % pcol_count)
            for source in raw[step]:
                wanted.append(jnp.where(held, source[tile // prow_count], 0.0))
    corners = lax.psum(jnp.stack(wanted), ("prow", "pcol"))
    corner = {}
    index = 0
    for tile in range(BLOCKS):
        for step in range(tile + 1):
            corner[tile, step] = (corners[index], corners[index + 1])
            index += 2

    def select_columns(panel):
        shaped = panel.reshape(col_tiles, ratio, width, width)
        return lax.dynamic_index_in_dim(shaped, pcol_index // prow_count, 1, keepdims=False)

    row_panels, col_panels = [], []
    for step in range(BLOCKS):
        owner = pcol_index == step % pcol_count
        got = lax.psum(tuple(jnp.where(owner, source, 0.0) for source in raw[step]), "pcol")
        row_panels.append(tuple(part.reshape(height, width) for part in got))
        picked = lax.psum(tuple(jnp.where(keeper, select_columns(part), 0.0) for part in got), "prow")
        col_panels.append(tuple(part.reshape(breadth, width) for part in picked))

    inverses = invert(jnp.stack([corner[step, step][1] for step in range(BLOCKS)]))

    cores = []
    tile_half = {}
    for step in range(BLOCKS):
        block = corner[step, step][0]
        for before in range(step):
            half, fact = tile_half[step, before]
            block = block - jnp.tril(product_trans(half, fact) + product_trans(fact, half))
        inverse = inverses[step]
        core = core_of(block, inverse)
        cores.append(core)
        for tile in range(step + 1, BLOCKS):
            piece, fact = corner[tile, step]
            for before in range(step):
                half_row, fact_row = tile_half[tile, before]
                half_col, fact_col = tile_half[step, before]
                piece = piece - product_trans(half_row, fact_col) - product_trans(fact_row, half_col)
            tile_half[tile, step] = (product_trans(piece, inverse) - 0.5 * product(fact, core), fact)

    def reduce_panels(panels, tile_of):
        halves, facts, finals = [], [], []
        for step in range(BLOCKS):
            panel, fact = panels[step]
            below = tile_of > step
            fact = jnp.where(below, fact, 0.0)
            for before in range(step):
                half_col, fact_col = tile_half[step, before]
                panel = panel - product_trans(
                    jnp.concatenate([halves[before], facts[before]], 1),
                    jnp.concatenate([fact_col, half_col], 1),
                )
            shared = product(fact, cores[step])
            half = jnp.where(below, product_trans(panel, inverses[step]), 0.0) - 0.5 * shared
            halves.append(half)
            facts.append(fact)
            finals.append(half - 0.5 * shared)
        return halves, facts, finals

    row_half, row_fact, finals = reduce_panels(row_panels, row_tile_of)
    col_half, col_fact, _ = reduce_panels(col_panels, col_tile_of)
    left = jnp.concatenate([part for pair in zip(row_half, row_fact) for part in pair], 1)
    right = jnp.concatenate([part for pair in zip(col_fact, col_half) for part in pair], 1)
    update = product_trans(left, right, high)
    local = matrix.reshape(height, breadth)
    local = local - jnp.where(elem_rows[:, None] >= elem_cols[None, :], update, 0.0)
    for step in range(BLOCKS):
        first = step // pcol_count * width
        current = local[:, first : first + width]
        diag_rows = jnp.tile(jnp.tril(cores[step]), (row_tiles, 1))
        column = jnp.where(row_tile_of == step, diag_rows, jnp.where(row_tile_of > step, finals[step], current))
        column = jnp.where(pcol_index == step % pcol_count, column, current)
        local = local.at[:, first : first + width].set(column)
    return local.reshape(row_tiles, 1, width, col_tiles, 1, width)


def solution(mesh):
    placed = P(None, "prow", None, None, "pcol", None)
    return jax.shard_map(on_device, mesh=mesh, in_specs=(placed, placed), out_specs=placed, check_vma=False)
```
